32 devices in a mesh: gx: 4 (over z), gy: 4 (over y, x), gz: 2 (over core).
Axes of the slice: x: 2, y: 2, z: 4, core: 2. Of those that a mesh axis runs over, the one named last changes fastest.
Arguments:
- east_wind: float32 [96, 512, 512], P('gz', 'gx', 'gy'), may hold values from -6 to 6
- north_wind: float32 [96, 512, 512], P('gz', 'gx', 'gy'), may hold values from -6 to 6
- vertical_wind: float32 [96, 512, 512], P('gz', 'gx', 'gy'), may hold values from -6 to 6
- geopotential: float32 [96, 512, 512], P('gz', 'gx', 'gy'), may hold values from -6 to 6
- pressure: float32 [96, 512, 512], P('gz', 'gx', 'gy'), may hold values from -6 to 6
- column_mass: float32 [512, 512], P('gx', 'gy'), may hold values from 0.5 to 2
Outputs:
- east_after: float32 [96, 512, 512], P('gz', 'gx', 'gy')
- north_after: float32 [96, 512, 512], P('gz', 'gx', 'gy')
- vertical_after: float32 [96, 512, 512], P('gz', 'gx', 'gy')
- geo_after: float32 [96, 512, 512], P('gz', 'gx', 'gy')
- pressure_after: float32 [96, 512, 512], P('gz', 'gx', 'gy')
The draws below stay inside these ranges and needn't reach their ends.
All inputs are finite; a program needn't handle non-finite values.
Results may differ from the reference program's by a relative error of at most 0.0003.
Values sent between devices are 32-bit elements; how exact they have to be, the bound alone decides.
A program may use at most 128 MiB of HBM per device.

```python
import math
import jax
import jax.numpy as jnp
from jax import lax

NZ = 96
ITERS = 3
NX = 512
NY = 512


def draw_vertical_wind(key, part):
    key_noise = jax.random.fold_in(key, 11)
    noise = jax.random.truncated_normal(key_noise, -6.0, 6.0, (NZ, NX, NY), jnp.float32)
    return noise


def steps_of(own_key, dims, shards, low, top_value):
    gain, own = 1.0, jax.random.fold_in(own_key, 6)
    for dim, blocks in shards:
        draws = jnp.exp(jax.random.uniform(jax.random.fold_in(own, dim), (blocks,), jnp.float32, low / len(shards), top_value / len(shards)))
        gain = gain * jnp.repeat(draws, dims[dim] // blocks).reshape([-1 if axis == dim else 1 for axis in range(len(dims))])
    return gain


def bell_draw(rng, shape, spread, reach, pieces=(), held_as=jnp.bfloat16):
    gain = steps_of(rng, shape, pieces, -0.22, 0.18) if pieces else 1.0
    drawn = jax.random.normal(rng, shape, jnp.float32) * spread * gain
    return jnp.minimum(jnp.maximum(drawn, -reach), reach).astype(held_as)


def setup_inputs(seed: int = 0) -> dict:
    seeds = jax.random.split(jax.random.key(seed), 7)
    return {
        "east_wind": bell_draw(seeds[0], (NZ, NX, NY), 1.0, 6.0, ((0, 2), (1, 4), (2, 4)), jnp.float32),
        "north_wind": bell_draw(seeds[1], (NZ, NX, NY), 1.0, 6.0, ((0, 2), (1, 4), (2, 4)), jnp.float32),
        "vertical_wind": draw_vertical_wind(jax.random.fold_in(seeds[6], 71), 0),
        "geopotential": bell_draw(seeds[3], (NZ, NX, NY), 1.0, 6.0, ((0, 2), (1, 4), (2, 4)), jnp.float32),
        "pressure": bell_draw(seeds[4], (NZ, NX, NY), 1.0, 6.0, ((0, 2), (1, 4), (2, 4)), jnp.float32),
        "column_mass": jnp.clip(jnp.exp(math.log(2.0) - 1.3862944 * jax.random.uniform(seeds[5], (NX, NY), jnp.float32) ** steps_of(seeds[5], (NX, NY), ((0, 4), (1, 4)), -0.2, 0.2)), 0.5, 2.0),
    }


horiz_push = 0.25
mass_flux = 0.2
level_push = 1.0
buoy_coupling = 0.5
geo_rate = 0.5
level_flux = 0.5
stiffness = 30.0


def centered(source, dim_index):
    return jnp.roll(source, -1, dim_index) - jnp.roll(source, 1, dim_index)


def level_diff(source):
    zeros_level = jnp.zeros_like(source[:1])
    shifted_up = jnp.concatenate([source[1:], zeros_level], 0)
    shifted_down = jnp.concatenate([zeros_level, source[:-1]], 0)
    return shifted_up - shifted_down


def column_solve(forcing, stiff_ratio):
    diagonal = 1.0 + 2.0 * stiff_ratio

    def forward(carried, forcing_row):
        coef_prev, rhs_prev = carried
        pivot_row = diagonal + stiff_ratio * coef_prev
        coef_next = -stiff_ratio / pivot_row
        rhs_next = (forcing_row + stiff_ratio * rhs_prev) / pivot_row
        return (coef_next, rhs_next), (coef_next, rhs_next)

    zeros_plane = jnp.zeros_like(stiff_ratio)
    _, (coefs, rhs_rows) = lax.scan(forward, (zeros_plane, zeros_plane), forcing)

    def backward(next_value, level_item):
        coef_row, rhs_row = level_item
        solved = rhs_row - coef_row * next_value
        return solved, solved

    _, solved = lax.scan(backward, zeros_plane, (coefs, rhs_rows), reverse=True)
    return solved


def reference(east_wind, north_wind, vertical_wind, geopotential, pressure, column_mass):
    stiff_ratio = stiffness * column_mass
    for substep in range(ITERS):
        east_wind = east_wind - horiz_push * centered(pressure, 1)
        north_wind = north_wind - horiz_push * centered(pressure, 2)
        divergence = centered(east_wind, 1) + centered(north_wind, 2)
        pressure_star = pressure - mass_flux * column_mass * divergence
        forcing = vertical_wind - level_push * level_diff(pressure_star) + buoy_coupling * geopotential
        vertical_wind = column_solve(forcing, stiff_ratio)
        geopotential = geopotential + geo_rate * vertical_wind
        pressure = pressure_star - level_flux * column_mass * level_diff(vertical_wind)
    return east_wind, north_wind, vertical_wind, geopotential, pressure
```

```python
import functools

import jax
import jax.numpy as jnp
from jax import lax
from jax.experimental import pallas as pl
from jax.experimental.pallas import tpu as pltpu
from jax.sharding import PartitionSpec as P

ITERS = 3
STIFF = 30.0
PAD = 8
ROWS = 16
UNROLL = 4


def roll(value, shift):
    if isinstance(shift, int):
        shift = shift % value.shape[1]
    return pltpu.roll(value, shift, 1)


def kernel(n, ni, nj, sizes, east_in, north_in, vert_in, geo_in, press_in, mass,
           east, north, vert, geo, press,
           pp, up, psum, dvg, mu_s, c_s, planes, bounds,
           row_out, row_in, col_out, col_in, z_out, z_in,
           load_sem, row_send, row_recv, col_send, col_recv, z_send, z_recv):
    nx, ny, nz = sizes
    ix, iy, iz = lax.axis_index("gx"), lax.axis_index("gy"), lax.axis_index("gz")
    xs = (lax.rem(ix + nx - 1, nx), lax.rem(ix + 1, nx))
    ys = (lax.rem(iy + ny - 1, ny), lax.rem(iy + 1, ny))

    loads = [
        pltpu.make_async_copy(press_in, pp.at[:, pl.ds(PAD, ni), :], load_sem.at[0]),
        pltpu.make_async_copy(east_in, up.at[:, pl.ds(PAD, ni), :], load_sem.at[1]),
        pltpu.make_async_copy(north_in, north, load_sem.at[2]),
        pltpu.make_async_copy(vert_in, vert, load_sem.at[3]),
        pltpu.make_async_copy(geo_in, geo, load_sem.at[4]),
    ]
    for load in loads:
        load.start()

    barrier = pltpu.get_barrier_semaphore()
    for t in range(2):
        pl.semaphore_signal(barrier, inc=1, device_id={"gx": xs[t]})
        pl.semaphore_signal(barrier, inc=1, device_id={"gy": ys[t]})
    for d in range(1, nz):
        pl.semaphore_signal(barrier, inc=1, device_id={"gz": lax.rem(iz + d, nz)})
    pl.semaphore_wait(barrier, 4 + nz - 1)

    def row_copy(slot, t):
        return pltpu.make_async_remote_copy(
            src_ref=row_out.at[slot, t], dst_ref=row_in.at[slot, 1 - t],
            send_sem=row_send.at[slot, t], recv_sem=row_recv.at[slot, 1 - t],
            device_id={"gx": xs[t]})

    def col_copy(slot, t):
        return pltpu.make_async_remote_copy(
            src_ref=col_out.at[slot, t], dst_ref=col_in.at[slot, 1 - t],
            send_sem=col_send.at[slot, t], recv_sem=col_recv.at[slot, 1 - t],
            device_id={"gy": ys[t]})

    def z_copy(slot, d):
        return pltpu.make_async_remote_copy(
            src_ref=z_out.at[slot], dst_ref=z_in.at[slot, d - 1],
            send_sem=z_send.at[slot, d - 1], recv_sem=z_recv.at[slot, d - 1],
            device_id={"gz": lax.rem(iz + d, nz)})

    lane = lax.broadcasted_iota(jnp.int32, (ROWS, nj), 1)
    pair = lane // 2

    def send_rows(slot, ref):
        row_out[slot, 0] = ref[:, PAD : PAD + 2, :]
        row_out[slot, 1] = ref[:, PAD + ni - 2 : PAD + ni, :]
        for t in range(2):
            row_copy(slot, t).start()

    def recv_rows(slot, ref):
        for t in range(2):
            row_copy(slot, t).wait()
        ref[:, PAD - 2 : PAD, :] = row_in[slot, 0]
        ref[:, PAD + ni : PAD + ni + 2, :] = row_in[slot, 1]

    def packed(value, k, packs):
        turned = roll(value, 2 * k + 2)
        return (jnp.where(pair == k + 1, turned, packs[0]), jnp.where(pair == k, turned, packs[1]))

    def strips(body):
        @pl.loop(0, ni // ROWS)
        def _(s):
            body(pl.multiple_of(s * ROWS, ROWS))

    def send_cols(slot, load_level):
        def body(r0):
            zero = jnp.zeros((ROWS, nj), jnp.float32)

            def group(q, packs):
                for e in range(UNROLL):
                    k = q * UNROLL + e
                    packs = packed(load_level(k, r0), k, packs)
                return packs

            packs = lax.fori_loop(0, n // UNROLL, group, (zero, zero))
            for t in range(2):
                col_out[slot, t, pl.ds(r0, ROWS), :] = packs[t]

        strips(body)
        for t in range(2):
            col_copy(slot, t).start()

    loads[0].wait()
    send_rows(0, pp)
    send_cols(0, lambda k, r0: pp[k, pl.ds(PAD + r0, ROWS), :])
    loads[1].wait()
    send_rows(ITERS, up)
    loads[2].wait()
    send_cols(ITERS, lambda k, r0: north[k, pl.ds(r0, ROWS), :])

    stiff = STIFF * mass[...]
    root = jnp.sqrt(1.0 + 4.0 * stiff)
    major = 0.5 * (1.0 + 2.0 * stiff + root)
    mu_s[...] = stiff / major
    c_s[...] = 1.0 / major
    planes[0] = jnp.log(stiff / major)
    planes[1] = major / root
    planes[2] = major / stiff

    recv_rows(0, pp)
    recv_rows(ITERS, up)
    for slot in (0, ITERS):
        for t in range(2):
            col_copy(slot, t).wait()
    loads[3].wait()
    loads[4].wait()

    def pass_one(it):
        def body(r0):
            rows = pl.ds(r0, ROWS)
            m, mu, c = mass[rows, :], mu_s[rows, :], c_s[rows, :]
            weak, strong = 0.05 * m, 0.2 * m
            left, right = col_in[it, 0, rows, :], col_in[it, 1, rows, :]
            if it == 0:
                vleft, vright = col_in[ITERS, 0, rows, :], col_in[ITERS, 1, rows, :]

            def star(k):
                at = pl.ds(PAD + r0, ROWS)
                p = pp[k, at, :]
                low = jnp.where(lane < 2, roll(left, (2 * nj - 2 * k) if isinstance(k, int) else nj - 2 * k), roll(p, 2))
                high = jnp.where(lane >= nj - 2, roll(right, nj - 4 - 2 * k), roll(p, nj - 2))
                total = (pp[k, pl.ds(PAD + r0 + 2, ROWS), :] + pp[k, pl.ds(PAD + r0 - 2, ROWS), :]) + (low + high) - 4.0 * p
                if it == 0:
                    v = north[k, rows, :]
                    vlow = jnp.where(lane < 1, roll(vleft, nj - 1 - 2 * k), roll(v, 1))
                    vhigh = jnp.where(lane >= nj - 1, roll(vright, nj - 3 - 2 * k), roll(v, nj - 1))
                    d = strong * (up[k, pl.ds(PAD + r0 + 1, ROWS), :] - up[k, pl.ds(PAD + r0 - 1, ROWS), :] + (vhigh - vlow))
                    psum[k, at, :] = p
                else:
                    d = dvg[k, rows, :]
                    psum[k, at, :] = psum[k, at, :] + p
                d = d - weak * total
                if it < ITERS - 1:
                    dvg[k, rows, :] = d
                ps = p - d
                press[k, rows, :] = ps
                return ps

            def sweep(k, above, below, state):
                y, dn, weight = state
                f = c * (vert[k, rows, :] + 0.5 * geo[k, rows, :] - (above - below))
                y = mu * y + f
                vert[k, rows, :] = y
                return y, dn + weight * f, weight * mu

            def steps(ks, carry):
                older, newer, state = carry
                for k in ks:
                    ps = star(k)
                    if not (isinstance(k, int) and k == 0):
                        state = sweep(k - 1, ps, older, state)
                    older, newer = newer, ps
                return older, newer, state

            zero = jnp.zeros((ROWS, nj), jnp.float32)
            carry = (zero, zero, (zero, zero, zero + 1.0))
            carry = steps(range(UNROLL), carry)
            planes_lo = press[0, rows, :]

            def group(q, carry):
                return steps([q * UNROLL + e for e in range(UNROLL)], carry)

            older, newer, state = lax.fori_loop(1, n // UNROLL, group, carry)
            y, dn, _ = sweep(n - 1, zero, older, state)
            z_out[it, 0, rows, :] = y
            z_out[it, 1, rows, :] = dn
            z_out[it, 2, rows, :] = c * planes_lo
            z_out[it, 3, rows, :] = c * newer

        strips(body)

    def interface(it):
        def body(r0):
            rows = pl.ds(r0, ROWS)
            mu, logmu, kappa, inv = mu_s[rows, :], planes[0, rows, :], planes[1, rows, :], planes[2, rows, :]
            zero = jnp.zeros((ROWS, nj), jnp.float32)

            def power(m):
                if not isinstance(m, int):
                    m = jnp.maximum(m, 0).astype(jnp.float32)
                return jnp.exp(m * logmu)

            near = power(n - 1)
            below, above, to_low, to_high = zero, zero, zero, zero
            pieces = {}

            def piece(d, which):
                if abs(d) >= nz:
                    return zero
                if d == 0:
                    return z_out[it, which, rows, :]
                value = z_in[it, (nz - d - 1) % nz if d > 0 else -d - 1, which, rows, :]
                inside = jnp.logical_and(iz + d >= 0, iz + d < nz)
                return jnp.where(inside, value, 0.0)

            own_up = own_dn = zero
            for d in range(-(nz - 1), nz):
                j = iz + d
                inside = jnp.logical_and(j >= 0, j < nz)
                under, over = piece(d - 1, 3), piece(d + 1, 2)
                upt = piece(d, 0) + near * under - over
                dnt = piece(d, 1) + under - near * over
                if d == 0:
                    own_up, own_dn = upt, dnt
                    delta_low, delta_high = under, over
                elif d < 0:
                    below = below + jnp.where(inside, power(n * (-1 - d)) * upt, 0.0)
                else:
                    above = above + jnp.where(inside, power(n * (d - 1)) * dnt, 0.0)
                to_low = to_low + jnp.where(inside, power(n * j + 1) * dnt, 0.0)
                to_high = to_high + jnp.where(inside, power(n * (nz - 1 - j) + 1) * upt, 0.0)
            q = power(n * nz + 1)
            scale = kappa / (1.0 - q * q)
            alpha = kappa * below + (q * to_high - to_low) * scale * power(n * iz)
            beta = kappa * above + (q * to_low - to_high) * scale * power(n * (nz - 1 - iz))
            far = power(n + 1)
            bounds[2, rows, :] = kappa * mu * own_dn + alpha + beta * far
            bounds[3, rows, :] = kappa * mu * own_up + beta + alpha * far
            alpha = alpha + kappa * delta_low * inv
            beta = beta - kappa * delta_high * inv
            bounds[0, rows, :] = kappa * mu * z_out[it, 0, rows, :] + beta
            bounds[1, rows, :] = alpha * power(n)

        strips(body)

    def pass_two(it):
        last = it == ITERS - 1

        def body(r0):
            rows = pl.ds(r0, ROWS)
            mu, inv = mu_s[rows, :], planes[2, rows, :]
            half = 0.5 * mass[rows, :]
            zero = jnp.zeros((ROWS, nj), jnp.float32)

            def finish(k, above, below, packs):
                p = press[k, rows, :] - half * (above - below)
                if last:
                    press[k, rows, :] = p
                    return packs
                pp[k, pl.ds(PAD + r0, ROWS), :] = p
                return packed(p, k, packs)

            def steps(ks, carry):
                x, h, older, newer, packs = carry
                for k in ks:
                    x = mu * x + vert[k, rows, :]
                    v = x + h
                    h = h * inv
                    vert[k, rows, :] = v
                    geo[k, rows, :] = geo[k, rows, :] + 0.5 * v
                    if not (isinstance(k, int) and k == n - 1):
                        packs = finish(k + 1, older, v, packs)
                    older, newer = newer, v
                return x, h, older, newer, packs

            top = bounds[3, rows, :]
            carry = (bounds[0, rows, :], bounds[1, rows, :], zero, top, (zero, zero))
            carry = steps([n - 1 - e for e in range(UNROLL)], carry)

            def group(q, carry):
                return steps([n - 1 - q * UNROLL - e for e in range(UNROLL)], carry)

            _, _, older, newer, packs = lax.fori_loop(1, n // UNROLL, group, carry)
            packs = finish(0, older, bounds[2, rows, :], packs)
            if not last:
                for t in range(2):
                    col_out[it + 1, t, rows, :] = packs[t]

        strips(body)

    def winds():
        def body(r0):
            rows = pl.ds(r0, ROWS)
            left = col_in[0, 0, rows, :]
            right = col_in[0, 1, rows, :]
            for it in range(1, ITERS):
                left = left + col_in[it, 0, rows, :]
                right = right + col_in[it, 1, rows, :]

            def group(q, carry):
                for e in range(UNROLL):
                    k = q * UNROLL + e
                    at = pl.ds(PAD + r0, ROWS)
                    p = psum[k, at, :]
                    east[k, rows, :] = up[k, at, :] - 0.25 * (
                        psum[k, pl.ds(PAD + r0 + 1, ROWS), :] - psum[k, pl.ds(PAD + r0 - 1, ROWS), :])
                    low = jnp.where(lane < 1, roll(left, nj - 1 - 2 * k), roll(p, 1))
                    high = jnp.where(lane >= nj - 1, roll(right, nj - 3 - 2 * k), roll(p, nj - 1))
                    north[k, rows, :] = north[k, rows, :] - 0.25 * (high - low)
                return carry

            lax.fori_loop(0, n // UNROLL, group, 0)

        strips(body)

    for it in range(ITERS):
        if it > 0:
            recv_rows(it, pp)
            for t in range(2):
                col_copy(it, t).wait()
        pass_one(it)
        for d in range(1, nz):
            z_copy(it, d).start()
        if it == ITERS - 1:
            for t, at in ((0, PAD - 2), (1, PAD + ni)):
                total = row_in[0, t]
                for slot in range(1, ITERS):
                    total = total + row_in[slot, t]
                psum[:, at : at + 2, :] = total
            winds()
        for d in range(1, nz):
            z_copy(it, d).wait()
        interface(it)
        pass_two(it)
        if it < ITERS - 1:
            send_rows(it + 1, pp)
            for t in range(2):
                col_copy(it + 1, t).start()


def local(sizes, east, north, vert, geo, press, mass):
    n, ni, nj = east.shape
    nz = sizes[2]
    f32 = jnp.float32
    slots = ITERS + 1
    field = pltpu.VMEM((n, ni, nj), f32)
    padded = pltpu.VMEM((n, ni + 2 * PAD, nj), f32)
    plane = pltpu.VMEM((ni, nj), f32)
    return pl.pallas_call(
        functools.partial(kernel, n, ni, nj, sizes),
        out_shape=[jax.ShapeDtypeStruct((n, ni, nj), f32)] * 5,
        in_specs=[pl.BlockSpec(memory_space=pl.ANY)] * 5 + [pl.BlockSpec(memory_space=pltpu.VMEM)],
        out_specs=[pl.BlockSpec(memory_space=pltpu.VMEM)] * 5,
        scratch_shapes=[
            padded, padded, padded, field, plane, plane,
            pltpu.VMEM((3, ni, nj), f32),
            pltpu.VMEM((4, ni, nj), f32),
            pltpu.VMEM((slots, 2, n, 2, nj), f32),
            pltpu.VMEM((slots, 2, n, 2, nj), f32),
            pltpu.VMEM((slots, 2, ni, nj), f32),
            pltpu.VMEM((slots, 2, ni, nj), f32),
            pltpu.VMEM((ITERS, 4, ni, nj), f32),
            pltpu.VMEM((ITERS, nz - 1, 4, ni, nj), f32),
            pltpu.SemaphoreType.DMA((5,)),
            pltpu.SemaphoreType.DMA((slots, 2)),
            pltpu.SemaphoreType.DMA((slots, 2)),
            pltpu.SemaphoreType.DMA((slots, 2)),
            pltpu.SemaphoreType.DMA((slots, 2)),
            pltpu.SemaphoreType.DMA((ITERS, nz - 1)),
            pltpu.SemaphoreType.DMA((ITERS, nz - 1)),
        ],
        compiler_params=pltpu.CompilerParams(
            collective_id=0, has_side_effects=True, vmem_limit_bytes=60 * 1024 * 1024),
    )(east, north, vert, geo, press, mass)


def solution(mesh):
    sizes = (mesh.shape["gx"], mesh.shape["gy"], mesh.shape["gz"])
    cube = P("gz", "gx", "gy")
    return jax.shard_map(
        functools.partial(local, sizes), mesh=mesh,
        in_specs=(cube,) * 5 + (P("gx", "gy"),), out_specs=(cube,) * 5, check_vma=False)
```

```python
import functools

import jax
import jax.numpy as jnp
from jax import lax
from jax.experimental import pallas as pl
from jax.experimental.pallas import tpu as pltpu
from jax.sharding import PartitionSpec as P

ITERS = 3
STIFF = 30.0
PAD = 8
ROWS = 16
UNROLL = 24


def roll(value, shift):
    if isinstance(shift, int):
        shift = shift % value.shape[1]
    return pltpu.roll(value, shift, 1)


def kernel(n, ni, nj, sizes, east_in, north_in, vert_in, geo_in, press_in, mass,
           east, north, vert, geo, press,
           pp, up, psum, dvg, mu_s, c_s, planes, bounds,
           row_out, row_in, col_out, col_in, z_out, z_in,
           load_sem, row_send, row_recv, col_send, col_recv, z_send, z_recv):
    nx, ny, nz = sizes
    unroll = max(u for u in range(1, UNROLL + 1) if n % u == 0)
    ix, iy, iz = lax.axis_index("gx"), lax.axis_index("gy"), lax.axis_index("gz")
    xs = (lax.rem(ix + nx - 1, nx), lax.rem(ix + 1, nx))
    ys = (lax.rem(iy + ny - 1, ny), lax.rem(iy + 1, ny))

    loads = [
        pltpu.make_async_copy(press_in, pp.at[:, pl.ds(PAD, ni), :], load_sem.at[0]),
        pltpu.make_async_copy(east_in, up.at[:, pl.ds(PAD, ni), :], load_sem.at[1]),
        pltpu.make_async_copy(north_in, north, load_sem.at[2]),
        pltpu.make_async_copy(vert_in, vert, load_sem.at[3]),
        pltpu.make_async_copy(geo_in, geo, load_sem.at[4]),
    ]
    for load in loads:
        load.start()

    barrier = pltpu.get_barrier_semaphore()
    for t in range(2):
        pl.semaphore_signal(barrier, inc=1, device_id={"gx": xs[t]})
        pl.semaphore_signal(barrier, inc=1, device_id={"gy": ys[t]})
    for d in range(1, nz):
        pl.semaphore_signal(barrier, inc=1, device_id={"gz": lax.rem(iz + d, nz)})
    pl.semaphore_wait(barrier, 4 + nz - 1)

    def row_copy(slot, t):
        return pltpu.make_async_remote_copy(
            src_ref=row_out.at[slot, t], dst_ref=row_in.at[slot, 1 - t],
            send_sem=row_send.at[slot, t], recv_sem=row_recv.at[slot, 1 - t],
            device_id={"gx": xs[t]})

    def col_copy(slot, t):
        return pltpu.make_async_remote_copy(
            src_ref=col_out.at[slot, t], dst_ref=col_in.at[slot, 1 - t],
            send_sem=col_send.at[slot, t], recv_sem=col_recv.at[slot, 1 - t],
            device_id={"gy": ys[t]})

    def z_copy(slot, d):
        return pltpu.make_async_remote_copy(
            src_ref=z_out.at[slot], dst_ref=z_in.at[slot, d - 1],
            send_sem=z_send.at[slot, d - 1], recv_sem=z_recv.at[slot, d - 1],
            device_id={"gz": lax.rem(iz + d, nz)})

    lane = lax.broadcasted_iota(jnp.int32, (ROWS, nj), 1)
    pair = lane // 2

    def send_rows(slot, ref):
        row_out[slot, 0] = ref[:, PAD : PAD + 2, :]
        row_out[slot, 1] = ref[:, PAD + ni - 2 : PAD + ni, :]
        for t in range(2):
            row_copy(slot, t).start()

    def recv_rows(slot, ref):
        for t in range(2):
            row_copy(slot, t).wait()
        ref[:, PAD - 2 : PAD, :] = row_in[slot, 0]
        ref[:, PAD + ni : PAD + ni + 2, :] = row_in[slot, 1]

    def packed(value, k, packs):
        turned = roll(value, 2 * k + 2)
        return (jnp.where(pair == k + 1, turned, packs[0]), jnp.where(pair == k, turned, packs[1]))

    def strips(body):
        @pl.loop(0, ni // ROWS)
        def _(s):
            body(pl.multiple_of(s * ROWS, ROWS))

    def send_cols(slot, load_level):
        def body(r0):
            zero = jnp.zeros((ROWS, nj), jnp.float32)

            def group(q, packs):
                for e in range(unroll):
                    k = q * unroll + e
                    packs = packed(load_level(k, r0), k, packs)
                return packs

            packs = lax.fori_loop(0, n // unroll, group, (zero, zero))
            for t in range(2):
                col_out[slot, t, pl.ds(r0, ROWS), :] = packs[t]

        strips(body)
        for t in range(2):
            col_copy(slot, t).start()

    loads[0].wait()
    send_rows(0, pp)
    send_cols(0, lambda k, r0: pp[k, pl.ds(PAD + r0, ROWS), :])
    loads[1].wait()
    send_rows(ITERS, up)
    loads[2].wait()
    send_cols(ITERS, lambda k, r0: north[k, pl.ds(r0, ROWS), :])

    stiff = STIFF * mass[...]
    root = jnp.sqrt(1.0 + 4.0 * stiff)
    major = 0.5 * (1.0 + 2.0 * stiff + root)
    mu_s[...] = stiff / major
    c_s[...] = 1.0 / major
    planes[0] = jnp.log(stiff / major)
    planes[1] = major / root
    planes[2] = major / stiff

    recv_rows(0, pp)
    recv_rows(ITERS, up)
    for slot in (0, ITERS):
        for t in range(2):
            col_copy(slot, t).wait()
    loads[3].wait()
    loads[4].wait()

    def pass_one(it):
        def body(r0):
            rows = pl.ds(r0, ROWS)
            m, mu, c = mass[rows, :], mu_s[rows, :], c_s[rows, :]
            weak, strong = 0.05 * m, 0.2 * m
            left, right = col_in[it, 0, rows, :], col_in[it, 1, rows, :]
            if it == 0:
                vleft, vright = col_in[ITERS, 0, rows, :], col_in[ITERS, 1, rows, :]

            def star(k):
                at = pl.ds(PAD + r0, ROWS)
                p = pp[k, at, :]
                low = jnp.where(lane < 2, roll(left, (2 * nj - 2 * k) if isinstance(k, int) else nj - 2 * k), roll(p, 2))
                high = jnp.where(lane >= nj - 2, roll(right, nj - 4 - 2 * k), roll(p, nj - 2))
                total = (pp[k, pl.ds(PAD + r0 + 2, ROWS), :] + pp[k, pl.ds(PAD + r0 - 2, ROWS), :]) + (low + high) - 4.0 * p
                if it == 0:
                    v = north[k, rows, :]
                    vlow = jnp.where(lane < 1, roll(vleft, nj - 1 - 2 * k), roll(v, 1))
                    vhigh = jnp.where(lane >= nj - 1, roll(vright, nj - 3 - 2 * k), roll(v, nj - 1))
                    d = strong * (up[k, pl.ds(PAD + r0 + 1, ROWS), :] - up[k, pl.ds(PAD + r0 - 1, ROWS), :] + (vhigh - vlow))
                    psum[k, at, :] = p
                else:
                    d = dvg[k, rows, :]
                    psum[k, at, :] = psum[k, at, :] + p
                d = d - weak * total
                if it < ITERS - 1:
                    dvg[k, rows, :] = d
                ps = p - d
                press[k, rows, :] = ps
                return ps

            def sweep(k, above, below, state):
                y, dn, weight = state
                f = c * (vert[k, rows, :] + 0.5 * geo[k, rows, :] - (above - below))
                y = mu * y + f
                vert[k, rows, :] = y
                return y, dn + weight * f, weight * mu

            def steps(ks, carry):
                older, newer, state = carry
                for k in ks:
                    ps = star(k)
                    if not (isinstance(k, int) and k == 0):
                        state = sweep(k - 1, ps, older, state)
                    older, newer = newer, ps
                return older, newer, state

            zero = jnp.zeros((ROWS, nj), jnp.float32)
            carry = (zero, zero, (zero, zero, zero + 1.0))
            carry = steps(range(unroll), carry)
            planes_lo = press[0, rows, :]

            def group(q, carry):
                return steps([q * unroll + e for e in range(unroll)], carry)

            older, newer, state = lax.fori_loop(1, n // unroll, group, carry)
            y, dn, _ = sweep(n - 1, zero, older, state)
            z_out[it, 0, rows, :] = y
            z_out[it, 1, rows, :] = dn
            z_out[it, 2, rows, :] = c * planes_lo
            z_out[it, 3, rows, :] = c * newer

        strips(body)

    def interface(it):
        def body(r0):
            rows = pl.ds(r0, ROWS)
            mu, logmu, kappa, inv = mu_s[rows, :], planes[0, rows, :], planes[1, rows, :], planes[2, rows, :]
            zero = jnp.zeros((ROWS, nj), jnp.float32)

            def power(m):
                if not isinstance(m, int):
                    m = jnp.maximum(m, 0).astype(jnp.float32)
                return jnp.exp(m * logmu)

            near = power(n - 1)
            below, above, to_low, to_high = zero, zero, zero, zero
            pieces = {}

            def piece(d, which):
                if abs(d) >= nz:
                    return zero
                if d == 0:
                    return z_out[it, which, rows, :]
                value = z_in[it, (nz - d - 1) % nz if d > 0 else -d - 1, which, rows, :]
                inside = jnp.logical_and(iz + d >= 0, iz + d < nz)
                return jnp.where(inside, value, 0.0)

            own_up = own_dn = zero
            for d in range(-(nz - 1), nz):
                j = iz + d
                inside = jnp.logical_and(j >= 0, j < nz)
                under, over = piece(d - 1, 3), piece(d + 1, 2)
                upt = piece(d, 0) + near * under - over
                dnt = piece(d, 1) + under - near * over
                if d == 0:
                    own_up, own_dn = upt, dnt
                    delta_low, delta_high = under, over
                elif d < 0:
                    below = below + jnp.where(inside, power(n * (-1 - d)) * upt, 0.0)
                else:
                    above = above + jnp.where(inside, power(n * (d - 1)) * dnt, 0.0)
                to_low = to_low + jnp.where(inside, power(n * j + 1) * dnt, 0.0)
                to_high = to_high + jnp.where(inside, power(n * (nz - 1 - j) + 1) * upt, 0.0)
            q = power(n * nz + 1)
            scale = kappa / (1.0 - q * q)
            alpha = kappa * below + (q * to_high - to_low) * scale * power(n * iz)
            beta = kappa * above + (q * to_low - to_high) * scale * power(n * (nz - 1 - iz))
            far = power(n + 1)
            bounds[2, rows, :] = kappa * mu * own_dn + alpha + beta * far
            bounds[3, rows, :] = kappa * mu * own_up + beta + alpha * far
            alpha = alpha + kappa * delta_low * inv
            beta = beta - kappa * delta_high * inv
            bounds[0, rows, :] = kappa * mu * z_out[it, 0, rows, :] + beta
            bounds[1, rows, :] = alpha * power(n)

        strips(body)

    def pass_two(it):
        last = it == ITERS - 1

        def body(r0):
            rows = pl.ds(r0, ROWS)
            mu, inv = mu_s[rows, :], planes[2, rows, :]
            half = 0.5 * mass[rows, :]
            zero = jnp.zeros((ROWS, nj), jnp.float32)

            def finish(k, above, below, packs):
                p = press[k, rows, :] - half * (above - below)
                if last:
                    press[k, rows, :] = p
                    return packs
                pp[k, pl.ds(PAD + r0, ROWS), :] = p
                return packed(p, k, packs)

            def steps(ks, carry):
                x, h, older, newer, packs = carry
                for k in ks:
                    x = mu * x + vert[k, rows, :]
                    v = x + h
                    h = h * inv
                    vert[k, rows, :] = v
                    geo[k, rows, :] = geo[k, rows, :] + 0.5 * v
                    if not (isinstance(k, int) and k == n - 1):
                        packs = finish(k + 1, older, v, packs)
                    older, newer = newer, v
                return x, h, older, newer, packs

            top = bounds[3, rows, :]
            carry = (bounds[0, rows, :], bounds[1, rows, :], zero, top, (zero, zero))
            carry = steps([n - 1 - e for e in range(unroll)], carry)

            def group(q, carry):
                return steps([n - 1 - q * unroll - e for e in range(unroll)], carry)

            _, _, older, newer, packs = lax.fori_loop(1, n // unroll, group, carry)
            packs = finish(0, older, bounds[2, rows, :], packs)
            if not last:
                for t in range(2):
                    col_out[it + 1, t, rows, :] = packs[t]

        strips(body)

    def winds():
        def body(r0):
            rows = pl.ds(r0, ROWS)
            left = col_in[0, 0, rows, :]
            right = col_in[0, 1, rows, :]
            for it in range(1, ITERS):
                left = left + col_in[it, 0, rows, :]
                right = right + col_in[it, 1, rows, :]

            def group(q, carry):
                for e in range(unroll):
                    k = q * unroll + e
                    at = pl.ds(PAD + r0, ROWS)
                    p = psum[k, at, :]
                    east[k, rows, :] = up[k, at, :] - 0.25 * (
                        psum[k, pl.ds(PAD + r0 + 1, ROWS), :] - psum[k, pl.ds(PAD + r0 - 1, ROWS), :])
                    low = jnp.where(lane < 1, roll(left, nj - 1 - 2 * k), roll(p, 1))
                    high = jnp.where(lane >= nj - 1, roll(right, nj - 3 - 2 * k), roll(p, nj - 1))
                    north[k, rows, :] = north[k, rows, :] - 0.25 * (high - low)
                return carry

            lax.fori_loop(0, n // unroll, group, 0)

        strips(body)

    for it in range(ITERS):
        if it > 0:
            recv_rows(it, pp)
            for t in range(2):
                col_copy(it, t).wait()
        pass_one(it)
        for d in range(1, nz):
            z_copy(it, d).start()
        if it == ITERS - 1:
            for t, at in ((0, PAD - 2), (1, PAD + ni)):
                total = row_in[0, t]
                for slot in range(1, ITERS):
                    total = total + row_in[slot, t]
                psum[:, at : at + 2, :] = total
            winds()
        for d in range(1, nz):
            z_copy(it, d).wait()
        interface(it)
        pass_two(it)
        if it < ITERS - 1:
            send_rows(it + 1, pp)
            for t in range(2):
                col_copy(it + 1, t).start()


def local(sizes, east, north, vert, geo, press, mass):
    n, ni, nj = east.shape
    nz = sizes[2]
    f32 = jnp.float32
    slots = ITERS + 1
    field = pltpu.VMEM((n, ni, nj), f32)
    padded = pltpu.VMEM((n, ni + 2 * PAD, nj), f32)
    plane = pltpu.VMEM((ni, nj), f32)
    return pl.pallas_call(
        functools.partial(kernel, n, ni, nj, sizes),
        out_shape=[pltpu.VMEM((n, ni, nj), f32)] * 5,
        in_specs=[pl.BlockSpec(memory_space=pl.ANY)] * 5 + [pl.BlockSpec(memory_space=pltpu.VMEM)],
        out_specs=[pl.BlockSpec(memory_space=pltpu.VMEM)] * 5,
        scratch_shapes=[
            padded, padded, padded, field, plane, plane,
            pltpu.VMEM((3, ni, nj), f32),
            pltpu.VMEM((4, ni, nj), f32),
            pltpu.VMEM((slots, 2, n, 2, nj), f32),
            pltpu.VMEM((slots, 2, n, 2, nj), f32),
            pltpu.VMEM((slots, 2, ni, nj), f32),
            pltpu.VMEM((slots, 2, ni, nj), f32),
            pltpu.VMEM((ITERS, 4, ni, nj), f32),
            pltpu.VMEM((ITERS, nz - 1, 4, ni, nj), f32),
            pltpu.SemaphoreType.DMA((5,)),
            pltpu.SemaphoreType.DMA((slots, 2)),
            pltpu.SemaphoreType.DMA((slots, 2)),
            pltpu.SemaphoreType.DMA((slots, 2)),
            pltpu.SemaphoreType.DMA((slots, 2)),
            pltpu.SemaphoreType.DMA((ITERS, nz - 1)),
            pltpu.SemaphoreType.DMA((ITERS, nz - 1)),
        ],
        compiler_params=pltpu.CompilerParams(
            collective_id=0, has_side_effects=True, vmem_limit_bytes=40 * 1024 * 1024),
    )(east, north, vert, geo, press, mass)


def solution(mesh):
    sizes = (mesh.shape["gx"], mesh.shape["gy"], mesh.shape["gz"])
    cube = P("gz", "gx", "gy")
    return jax.shard_map(
        functools.partial(local, sizes), mesh=mesh,
        in_specs=(cube,) * 5 + (P("gx", "gy"),), out_specs=(cube,) * 5, check_vma=False)
```

```python
import functools

import jax
import jax.numpy as jnp
from jax import lax
from jax.experimental import pallas as pl
from jax.experimental.pallas import tpu as pltpu
from jax.sharding import PartitionSpec as P

ITERS = 3
STIFF = 30.0
PAD = 8
ROWS = 16
PARTS = 2
UNROLL = 24


def roll(value, shift):
    if isinstance(shift, int):
        shift = shift % value.shape[1]
    return pltpu.roll(value, shift, 1)


def kernel(n, ni, nj, sizes, east_in, north_in, vert_in, geo_in, press_in, mass,
           east, north, vert, geo, press,
           pp, up, psum, dvg, mu_s, c_s, planes, bounds,
           row_out, row_in, col_out, col_in, z_out, z_in,
           load_sem, row_send, row_recv, col_send, col_recv, z_send, z_recv):
    nx, ny, nz = sizes
    unroll = max(u for u in range(2, UNROLL + 1) if n % u == 0 and u % 2 == 0)
    ix, iy, iz = lax.axis_index("gx"), lax.axis_index("gy"), lax.axis_index("gz")
    xs = (lax.rem(ix + nx - 1, nx), lax.rem(ix + 1, nx))
    ys = (lax.rem(iy + ny - 1, ny), lax.rem(iy + 1, ny))

    loads = [
        pltpu.make_async_copy(press_in, pp.at[:, pl.ds(PAD, ni), :], load_sem.at[0]),
        pltpu.make_async_copy(east_in, up.at[:, pl.ds(PAD, ni), :], load_sem.at[1]),
        pltpu.make_async_copy(north_in, north, load_sem.at[2]),
        pltpu.make_async_copy(vert_in, vert, load_sem.at[3]),
        pltpu.make_async_copy(geo_in, geo, load_sem.at[4]),
    ]
    for load in loads:
        load.start()

    barrier = pltpu.get_barrier_semaphore()
    for t in range(2):
        pl.semaphore_signal(barrier, inc=1, device_id={"gx": xs[t]})
        pl.semaphore_signal(barrier, inc=1, device_id={"gy": ys[t]})
    for d in range(1, nz):
        pl.semaphore_signal(barrier, inc=1, device_id={"gz": lax.rem(iz + d, nz)})
    pl.semaphore_wait(barrier, 4 + nz - 1)

    def row_copy(slot, t):
        return pltpu.make_async_remote_copy(
            src_ref=row_out.at[slot, t], dst_ref=row_in.at[slot, 1 - t],
            send_sem=row_send.at[slot, t], recv_sem=row_recv.at[slot, 1 - t],
            device_id={"gx": xs[t]})

    span = ni // PARTS

    def part_rows(h):
        return pl.ds(pl.multiple_of(h * span, span), span)

    def col_copy(slot, t, h):
        return pltpu.make_async_remote_copy(
            src_ref=col_out.at[slot, t, part_rows(h), :], dst_ref=col_in.at[slot, 1 - t, part_rows(h), :],
            send_sem=col_send.at[slot, t, h], recv_sem=col_recv.at[slot, 1 - t, h],
            device_id={"gy": ys[t]})

    def z_copy(slot, d, h):
        return pltpu.make_async_remote_copy(
            src_ref=z_out.at[slot, :, part_rows(h), :], dst_ref=z_in.at[slot, d - 1, :, part_rows(h), :],
            send_sem=z_send.at[slot, d - 1, h], recv_sem=z_recv.at[slot, d - 1, h],
            device_id={"gz": lax.rem(iz + d, nz)})

    lane = lax.broadcasted_iota(jnp.int32, (ROWS, nj), 1)
    pair = lane // 2

    def merged(left, right, width):
        left, right = roll(left, width), roll(right, nj - width)
        even = pair % 2 == 0
        return jnp.where(even, right, left), jnp.where(even, left, right)

    def send_rows(slot, ref):
        row_out[slot, 0] = ref[:, PAD : PAD + 2, :]
        row_out[slot, 1] = ref[:, PAD + ni - 2 : PAD + ni, :]
        for t in range(2):
            row_copy(slot, t).start()

    def recv_rows(slot, ref):
        for t in range(2):
            row_copy(slot, t).wait()
        ref[:, PAD - 2 : PAD, :] = row_in[slot, 0]
        ref[:, PAD + ni : PAD + ni + 2, :] = row_in[slot, 1]

    def packed(value, k, packs):
        turned = roll(value, 2 * k + 2)
        return (jnp.where(pair == k + 1, turned, packs[0]), jnp.where(pair == k, turned, packs[1]))

    def strips(body, h=None):
        count = (ni if h is None else span) // ROWS
        first = 0 if h is None else h * count

        @pl.loop(0, count)
        def _(s):
            body(pl.multiple_of((first + s) * ROWS, ROWS))

    def send_cols(slot, load_level):
        def body(r0):
            zero = jnp.zeros((ROWS, nj), jnp.float32)

            def group(q, packs):
                for e in range(unroll):
                    k = q * unroll + e
                    packs = packed(load_level(k, r0), k, packs)
                return packs

            packs = lax.fori_loop(0, n // unroll, group, (zero, zero))
            for t in range(2):
                col_out[slot, t, pl.ds(r0, ROWS), :] = packs[t]

        strips(body)
        for h in range(PARTS):
            for t in range(2):
                col_copy(slot, t, h).start()

    loads[0].wait()
    send_rows(0, pp)
    send_cols(0, lambda k, r0: pp[k, pl.ds(PAD + r0, ROWS), :])
    loads[1].wait()
    send_rows(ITERS, up)
    loads[2].wait()
    send_cols(ITERS, lambda k, r0: north[k, pl.ds(r0, ROWS), :])

    stiff = STIFF * mass[...]
    root = jnp.sqrt(1.0 + 4.0 * stiff)
    major = 0.5 * (1.0 + 2.0 * stiff + root)
    mu_s[...] = stiff / major
    c_s[...] = 1.0 / major
    planes[0] = jnp.log(stiff / major)
    planes[1] = major / root
    planes[2] = major / stiff

    recv_rows(0, pp)
    recv_rows(ITERS, up)
    for slot in (0, ITERS):
        for t in range(2):
            for h in range(PARTS):
                col_copy(slot, t, h).wait()
    loads[3].wait()
    loads[4].wait()

    def pass_one(it, h):
        def body(r0):
            rows = pl.ds(r0, ROWS)
            m, mu, c = mass[rows, :], mu_s[rows, :], c_s[rows, :]
            weak, strong = 0.05 * m, 0.2 * m
            left, right = col_in[it, 0, rows, :], col_in[it, 1, rows, :]
            ends = merged(left, right, 2)
            if it == 0:
                vends = merged(col_in[ITERS, 0, rows, :], col_in[ITERS, 1, rows, :], 1)

            def star(k, parity):
                end = roll(ends[parity], nj - 2 - 2 * k)
                at = pl.ds(PAD + r0, ROWS)
                p = pp[k, at, :]
                low = jnp.where(lane < 2, end, roll(p, 2))
                high = jnp.where(lane >= nj - 2, end, roll(p, nj - 2))
                total = (pp[k, pl.ds(PAD + r0 + 2, ROWS), :] + pp[k, pl.ds(PAD + r0 - 2, ROWS), :]) + (low + high) - 4.0 * p
                if it == 0:
                    v = north[k, rows, :]
                    vend = roll(vends[parity], nj - 2 - 2 * k)
                    vlow = jnp.where(lane < 1, vend, roll(v, 1))
                    vhigh = jnp.where(lane >= nj - 1, vend, roll(v, nj - 1))
                    d = strong * (up[k, pl.ds(PAD + r0 + 1, ROWS), :] - up[k, pl.ds(PAD + r0 - 1, ROWS), :] + (vhigh - vlow))
                    psum[k, at, :] = p
                else:
                    d = dvg[k, rows, :]
                    psum[k, at, :] = psum[k, at, :] + p
                d = d - weak * total
                if it < ITERS - 1:
                    dvg[k, rows, :] = d
                ps = p - d
                press[k, rows, :] = ps
                return ps

            def sweep(k, above, below, state):
                y, dn, weight = state
                f = c * (vert[k, rows, :] + 0.5 * geo[k, rows, :] - (above - below))
                y = mu * y + f
                vert[k, rows, :] = y
                return y, dn + weight * f, weight * mu

            def steps(ks, carry):
                older, newer, state = carry
                for e, k in enumerate(ks):
                    ps = star(k, e % 2)
                    if not (isinstance(k, int) and k == 0):
                        state = sweep(k - 1, ps, older, state)
                    older, newer = newer, ps
                return older, newer, state

            zero = jnp.zeros((ROWS, nj), jnp.float32)
            carry = (zero, zero, (zero, zero, zero + 1.0))
            carry = steps(range(unroll), carry)
            planes_lo = press[0, rows, :]

            def group(q, carry):
                return steps([q * unroll + e for e in range(unroll)], carry)

            older, newer, state = lax.fori_loop(1, n // unroll, group, carry)
            y, dn, _ = sweep(n - 1, zero, older, state)
            z_out[it, 0, rows, :] = y
            z_out[it, 1, rows, :] = dn
            z_out[it, 2, rows, :] = c * planes_lo
            z_out[it, 3, rows, :] = c * newer

        strips(body, h)

    def interface(it, h):
        def body(r0):
            rows = pl.ds(r0, ROWS)
            mu, logmu, kappa, inv = mu_s[rows, :], planes[0, rows, :], planes[1, rows, :], planes[2, rows, :]
            zero = jnp.zeros((ROWS, nj), jnp.float32)

            def power(m):
                if not isinstance(m, int):
                    m = jnp.maximum(m, 0).astype(jnp.float32)
                return jnp.exp(m * logmu)

            near = power(n - 1)
            below, above, to_low, to_high = zero, zero, zero, zero
            pieces = {}

            def piece(d, which):
                if abs(d) >= nz:
                    return zero
                if d == 0:
                    return z_out[it, which, rows, :]
                value = z_in[it, (nz - d - 1) % nz if d > 0 else -d - 1, which, rows, :]
                inside = jnp.logical_and(iz + d >= 0, iz + d < nz)
                return jnp.where(inside, value, 0.0)

            own_up = own_dn = zero
            for d in range(-(nz - 1), nz):
                j = iz + d
                inside = jnp.logical_and(j >= 0, j < nz)
                under, over = piece(d - 1, 3), piece(d + 1, 2)
                upt = piece(d, 0) + near * under - over
                dnt = piece(d, 1) + under - near * over
                if d == 0:
                    own_up, own_dn = upt, dnt
                    delta_low, delta_high = under, over
                elif d < 0:
                    below = below + jnp.where(inside, power(n * (-1 - d)) * upt, 0.0)
                else:
                    above = above + jnp.where(inside, power(n * (d - 1)) * dnt, 0.0)
                to_low = to_low + jnp.where(inside, power(n * j + 1) * dnt, 0.0)
                to_high = to_high + jnp.where(inside, power(n * (nz - 1 - j) + 1) * upt, 0.0)
            q = power(n * nz + 1)
            scale = kappa / (1.0 - q * q)
            alpha = kappa * below + (q * to_high - to_low) * scale * power(n * iz)
            beta = kappa * above + (q * to_low - to_high) * scale * power(n * (nz - 1 - iz))
            far = power(n + 1)
            bounds[2, rows, :] = kappa * mu * own_dn + alpha + beta * far
            bounds[3, rows, :] = kappa * mu * own_up + beta + alpha * far
            alpha = alpha + kappa * delta_low * inv
            beta = beta - kappa * delta_high * inv
            bounds[0, rows, :] = kappa * mu * z_out[it, 0, rows, :] + beta
            bounds[1, rows, :] = alpha * power(n)

        strips(body, h)

    def pass_two(it, h):
        last = it == ITERS - 1

        def body(r0):
            rows = pl.ds(r0, ROWS)
            mu, inv = mu_s[rows, :], planes[2, rows, :]
            half = 0.5 * mass[rows, :]
            zero = jnp.zeros((ROWS, nj), jnp.float32)

            def finish(k, above, below, packs):
                p = press[k, rows, :] - half * (above - below)
                if last:
                    press[k, rows, :] = p
                    return packs
                pp[k, pl.ds(PAD + r0, ROWS), :] = p
                return packed(p, k, packs)

            def steps(ks, carry):
                x, h, older, newer, packs = carry
                for k in ks:
                    x = mu * x + vert[k, rows, :]
                    v = x + h
                    h = h * inv
                    vert[k, rows, :] = v
                    geo[k, rows, :] = geo[k, rows, :] + 0.5 * v
                    if not (isinstance(k, int) and k == n - 1):
                        packs = finish(k + 1, older, v, packs)
                    older, newer = newer, v
                return x, h, older, newer, packs

            top = bounds[3, rows, :]
            carry = (bounds[0, rows, :], bounds[1, rows, :], zero, top, (zero, zero))
            carry = steps([n - 1 - e for e in range(unroll)], carry)

            def group(q, carry):
                return steps([n - 1 - q * unroll - e for e in range(unroll)], carry)

            _, _, older, newer, packs = lax.fori_loop(1, n // unroll, group, carry)
            packs = finish(0, older, bounds[2, rows, :], packs)
            if not last:
                for t in range(2):
                    col_out[it + 1, t, rows, :] = packs[t]

        strips(body, h)

    def winds():
        def body(r0):
            rows = pl.ds(r0, ROWS)
            left = col_in[0, 0, rows, :]
            right = col_in[0, 1, rows, :]
            for it in range(1, ITERS):
                left = left + col_in[it, 0, rows, :]
                right = right + col_in[it, 1, rows, :]

            ends = merged(left, right, 1)

            def group(q, carry):
                for e in range(unroll):
                    k = q * unroll + e
                    end = roll(ends[e % 2], nj - 2 - 2 * k)
                    at = pl.ds(PAD + r0, ROWS)
                    p = psum[k, at, :]
                    east[k, rows, :] = up[k, at, :] - 0.25 * (
                        psum[k, pl.ds(PAD + r0 + 1, ROWS), :] - psum[k, pl.ds(PAD + r0 - 1, ROWS), :])
                    low = jnp.where(lane < 1, end, roll(p, 1))
                    high = jnp.where(lane >= nj - 1, end, roll(p, nj - 1))
                    north[k, rows, :] = north[k, rows, :] - 0.25 * (high - low)
                return carry

            lax.fori_loop(0, n // unroll, group, 0)

        strips(body)

    for it in range(ITERS):
        if it > 0:
            recv_rows(it, pp)

        @pl.loop(0, PARTS)
        def _(h, it=it):
            if it > 0:
                for t in range(2):
                    col_copy(it, t, h).wait()
            pass_one(it, h)
            for d in range(1, nz):
                z_copy(it, d, h).start()

        if it == ITERS - 1:
            for t, at in ((0, PAD - 2), (1, PAD + ni)):
                total = row_in[0, t]
                for slot in range(1, ITERS):
                    total = total + row_in[slot, t]
                psum[:, at : at + 2, :] = total
            winds()

        @pl.loop(0, PARTS)
        def _(h, it=it):
            for d in range(1, nz):
                z_copy(it, d, h).wait()
            interface(it, h)
            pass_two(it, h)
            if it < ITERS - 1:
                for t in range(2):
                    col_copy(it + 1, t, h).start()

        if it < ITERS - 1:
            send_rows(it + 1, pp)


def local(sizes, east, north, vert, geo, press, mass):
    n, ni, nj = east.shape
    nz = sizes[2]
    f32 = jnp.float32
    slots = ITERS + 1
    field = pltpu.VMEM((n, ni, nj), f32)
    padded = pltpu.VMEM((n, ni + 2 * PAD, nj), f32)
    plane = pltpu.VMEM((ni, nj), f32)
    return pl.pallas_call(
        functools.partial(kernel, n, ni, nj, sizes),
        out_shape=[pltpu.VMEM((n, ni, nj), f32)] * 5,
        in_specs=[pl.BlockSpec(memory_space=pl.ANY)] * 5 + [pl.BlockSpec(memory_space=pltpu.VMEM)],
        out_specs=[pl.BlockSpec(memory_space=pltpu.VMEM)] * 5,
        scratch_shapes=[
            padded, padded, padded, field, plane, plane,
            pltpu.VMEM((3, ni, nj), f32),
            pltpu.VMEM((4, ni, nj), f32),
            pltpu.VMEM((slots, 2, n, 2, nj), f32),
            pltpu.VMEM((slots, 2, n, 2, nj), f32),
            pltpu.VMEM((slots, 2, ni, nj), f32),
            pltpu.VMEM((slots, 2, ni, nj), f32),
            pltpu.VMEM((ITERS, 4, ni, nj), f32),
            pltpu.VMEM((ITERS, nz - 1, 4, ni, nj), f32),
            pltpu.SemaphoreType.DMA((5,)),
            pltpu.SemaphoreType.DMA((slots, 2)),
            pltpu.SemaphoreType.DMA((slots, 2)),
            pltpu.SemaphoreType.DMA((slots, 2, PARTS)),
            pltpu.SemaphoreType.DMA((slots, 2, PARTS)),
            pltpu.SemaphoreType.DMA((ITERS, nz - 1, PARTS)),
            pltpu.SemaphoreType.DMA((ITERS, nz - 1, PARTS)),
        ],
        compiler_params=pltpu.CompilerParams(
            collective_id=0, has_side_effects=True, vmem_limit_bytes=40 * 1024 * 1024),
    )(east, north, vert, geo, press, mass)


def solution(mesh):
    sizes = (mesh.shape["gx"], mesh.shape["gy"], mesh.shape["gz"])
    cube = P("gz", "gx", "gy")
    return jax.shard_map(
        functools.partial(local, sizes), mesh=mesh,
        in_specs=(cube,) * 5 + (P("gx", "gy"),), out_specs=(cube,) * 5, check_vma=False)
```
